32 devices in a mesh: date: 8 (over z, x), pix: 4 (over y, core).
Axes of the slice: x: 2, y: 2, z: 4, core: 2. Of those that a mesh axis runs over, the one named last changes fastest.
Arguments:
- stack: bfloat16 [8, 10, 32, 2048], P('date', None, 'pix'), may hold values from -4 to 12
- cloud: int32 [8, 32, 2048], P('date', 'pix'), may hold values 0 or 1
Outputs:
- composite: float32 [10, 32, 2048], P(None, 'pix')
The draws below stay inside these ranges and needn't reach their ends.
All inputs are finite; a program needn't handle non-finite values. No bound on the sum of `cloud` on one device may be relied on, other than what follows from the above.
Results may differ from the reference program's by a relative error of at most 0.0003.
Values may be sent and summed in bfloat16 or wider, within the bound.
No kernel may reach another device: no remote copies, remote signals or barrier semaphores. Data moves between devices by JAX's collectives and lax.ppermute only.
A program may use at most 64 MiB of HBM per device.

```python
import jax
import jax.numpy as jnp
from jax import lax

BANDS = 10
ROWS_DEV = 8
COLS = 2048
ITERS = 2
DATES = 8
NROWS = 32


def draw_stack(key, part):
    keys = jax.random.split(jax.random.fold_in(key, 17), 5)
    rows = jnp.arange(NROWS, dtype=jnp.float32)
    bright = 1.0 + 2.0 * rows / max(NROWS - 1, 1)
    band_base = jax.random.uniform(keys[0], (BANDS,), jnp.float32, 0.5, 1.5)
    surface = jax.random.normal(keys[1], (BANDS, NROWS, COLS), jnp.float32)
    noise = jax.random.normal(keys[2], (DATES, BANDS, NROWS, COLS), jnp.float32)
    hazy = jax.random.bernoulli(keys[3], 0.1, (DATES, 1, NROWS, COLS)).astype(jnp.float32)
    haze = hazy * jax.random.uniform(keys[4], (DATES, 1, NROWS, COLS), jnp.float32, 1.0, 3.0)
    ground = bright[None, :, None] * band_base[:, None, None] * (1.0 + 0.3 * surface)
    values = ground[None] + noise + haze
    return jnp.clip(values, -4.0, 12.0).astype(jnp.bfloat16)


def place_ends(drawn, key, least, high):
    spot = [jax.random.randint(jax.random.fold_in(key, axis), (), 0, length) for axis, length in enumerate(drawn.shape)]
    longest = drawn.shape.index(max(drawn.shape))
    next_to = spot[:longest] + [(spot[longest] + 1) % drawn.shape[longest]] + spot[longest + 1:]
    return drawn.at[tuple(spot)].set(least).at[tuple(next_to)].set(high)


def setup_inputs(seed: int = 0) -> dict:
    seeds = jax.random.split(jax.random.key(seed), 3)
    return {
        "stack": draw_stack(jax.random.fold_in(seeds[2], 71), 0),
        "cloud": place_ends((jax.random.randint(seeds[1], (DATES, NROWS, COLS), 0, 4) < 3).astype(jnp.int32), jax.random.fold_in(seeds[1], 1), 0, 1),
    }


delta_sq = 0.01
eps = 1e-05

def clear_flags(cloud):
    cloudy = (1 - cloud).astype(jnp.float32)
    padded = jnp.pad(cloudy, ((0, 0), (1, 1), (1, 1)))
    near = jnp.maximum(padded[:, 1:-1, 1:-1], padded[:, 2:, 1:-1])
    near = jnp.maximum(near, padded[:, :-2, 1:-1])
    near = jnp.maximum(near, padded[:, 1:-1, 2:])
    near = jnp.maximum(near, padded[:, 1:-1, :-2])
    return 1.0 - near

def median_block(block, valid):
    values = block.astype(jnp.float32)
    median = jnp.zeros(values.shape[1:], jnp.float32)
    for step in range(ITERS + 1):
        if step == 0:
            weight = valid
        else:
            diff = values - median[None]
            weight = valid / jnp.sqrt(lax.optimization_barrier(jnp.sum(diff * diff, axis=1)) + delta_sq)
        numer = lax.optimization_barrier(jnp.sum(weight[:, None] * values, axis=0))
        denom = lax.optimization_barrier(jnp.sum(weight, axis=0))
        median = (numer + median) / (denom + 1.0)
    return median

def reference(stack, cloud):
    valid = clear_flags(cloud)
    blocks = NROWS // ROWS_DEV

    def one_block(index):
        start = (index * ROWS_DEV).astype(jnp.int32)
        part = lax.dynamic_slice_in_dim(stack, start, ROWS_DEV, 2)
        flags = lax.dynamic_slice_in_dim(valid, start, ROWS_DEV, 1)
        return median_block(part, flags)
    pieces = lax.map(one_block, jnp.arange(blocks, dtype=jnp.int32))
    median = jnp.transpose(pieces, (1, 0, 2, 3)).reshape(BANDS, NROWS, COLS)
    count = NROWS * COLS
    mean = lax.optimization_barrier(jnp.sum(median, axis=(1, 2))) / count
    var = lax.optimization_barrier(jnp.sum(median * median, axis=(1, 2))) / count - mean * mean
    return (median - mean[:, None, None]) / jnp.sqrt(var[:, None, None] + eps)
```

```python
import jax
import jax.numpy as jnp
from jax import lax
from jax.sharding import PartitionSpec as P

ITERS = 2


delta_sq = 0.01
eps = 1e-05


def with_halo(cells, axis, dim):
    count = lax.axis_size(axis)
    ends = count - 1
    head = lax.slice_in_dim(cells, 0, 1, axis=dim)
    tail = lax.slice_in_dim(cells, cells.shape[dim] - 1, cells.shape[dim], axis=dim)
    return jnp.concatenate(
        [
            lax.ppermute(tail, axis, [(i, (i + 1) % count) for i in range(ends)]),
            cells,
            lax.ppermute(head, axis, [((i + 1) % count, i) for i in range(ends)]),
        ],
        axis=dim,
    )


def weiszfeld(values, valid):
    median = jnp.zeros(values.shape[1:], jnp.float32)
    for step in range(ITERS + 1):
        if step == 0:
            weight = valid
        else:
            diff = values - median[None]
            weight = valid / jnp.sqrt(jnp.sum(diff * diff, axis=1) + delta_sq)
        numer = jnp.sum(weight[:, None] * values, axis=0)
        denom = jnp.sum(weight, axis=0)
        median = (numer + median) / (denom + 1.0)
    return median


def body(stack, cloud):
    bands = stack.shape[1]
    rows = stack.shape[2]
    cols = stack.shape[3]
    cloudy = (1 - cloud).astype(jnp.bfloat16)
    rimmed = with_halo(cloudy, "pix", 1).astype(jnp.float32)
    padded = jnp.pad(rimmed, ((0, 0), (0, 0), (1, 1)))
    near = jnp.maximum(padded[:, 1:-1, 1:-1], padded[:, 2:, 1:-1])
    near = jnp.maximum(near, padded[:, :-2, 1:-1])
    near = jnp.maximum(near, padded[:, 1:-1, 2:])
    near = jnp.maximum(near, padded[:, 1:-1, :-2])
    valid = (1.0 - near).astype(jnp.bfloat16)
    planes = jnp.concatenate([stack, valid[:, None]], axis=1)
    planes = lax.all_to_all(planes, "date", 3, 0, tiled=True).astype(jnp.float32)
    median = weiszfeld(planes[:, :bands], planes[:, bands])
    median = lax.all_gather(median, "date", axis=2, tiled=True)
    count = lax.axis_size("pix") * rows * cols
    sums = lax.psum((jnp.sum(median, axis=(1, 2)), jnp.sum(median * median, axis=(1, 2))), "pix")
    mean = sums[0] / count
    var = sums[1] / count - mean * mean
    return (median - mean[:, None, None]) / jnp.sqrt(var[:, None, None] + eps)


def solution(mesh):
    placed = (P("date", None, "pix", None), P("date", "pix", None))
    return jax.shard_map(
        body, mesh=mesh, in_specs=placed, out_specs=P(None, "pix", None), check_vma=False
    )
```

```python
import functools

import jax
import jax.numpy as jnp
from jax import lax
from jax.experimental import pallas as pl
from jax.experimental.pallas import tpu as pltpu
from jax.sharding import PartitionSpec as P

ITERS = 2
LANES = 128

delta_sq = 0.01
eps = 1e-05


def row_permutes(head, tail, axis):
    count = lax.axis_size(axis)
    ends = count - 1
    above = lax.ppermute(tail, axis, [(i, i + 1) for i in range(ends)])
    below = lax.ppermute(head, axis, [(i + 1, i) for i in range(ends)])
    return above, below


def swap(x, axis, bits):
    count = lax.axis_size(axis)
    return lax.ppermute(x, axis, [(i, i ^ bits) for i in range(count)])


VMEM = pl.BlockSpec(memory_space=pltpu.VMEM)


def call(kernel, outs, name, flops=2_000_000, **kwargs):
    def run(*args):
        return pl.pallas_call(
            kernel,
            out_shape=outs,
            in_specs=[VMEM] * len(args),
            out_specs=jax.tree.map(lambda _: VMEM, outs),
            compiler_params=pltpu.CompilerParams(vmem_limit_bytes=16 * 2**20),
            cost_estimate=pl.CostEstimate(flops=flops, bytes_accessed=0, transcendentals=0),
            name=name,
            **kwargs,
        )(*args)

    return run


def valid_flags(cloud, above, below):
    cloudy = (1 - cloud).astype(jnp.float32)
    rows, cols = cloudy.shape
    up = jnp.concatenate([above, cloudy[:-1]], axis=0)
    down = jnp.concatenate([cloudy[1:], below], axis=0)
    edge = jnp.zeros((rows, 1), jnp.float32)
    left = jnp.concatenate([edge, cloudy[:, :-1]], axis=1)
    right = jnp.concatenate([cloudy[:, 1:], edge], axis=1)
    near = jnp.maximum(jnp.maximum(jnp.maximum(cloudy, up), jnp.maximum(down, left)), right)
    return 1.0 - near


def pack_kernel(stack, cloud, above, below, *refs):
    outs, flags = refs[:-1], refs[-1]
    bands = stack.shape[1]
    width = outs[0].shape[-1]
    me = lax.axis_index("date")
    flags[...] = valid_flags(
        cloud[0], above[0].astype(jnp.float32), below[0].astype(jnp.float32)
    ).astype(jnp.bfloat16)
    for k, out in enumerate(outs):
        cols = pl.ds(pl.multiple_of((me ^ k) * width, width), width)
        for band in range(bands):
            out[band] = stack[0, band, :, cols]
        out[bands] = flags[:, cols]


def update_kernel(*refs):
    parts, out = refs[:-1], refs[-1]
    bands = out.shape[0]
    for first in range(0, out.shape[2], LANES):
        cols = pl.ds(first, LANES)
        median = None
        for step in range(ITERS + 1):
            numer, denom = [None] * bands, None
            for part in parts:
                values = [part[band, :, cols].astype(jnp.float32) for band in range(bands)]
                weight = part[bands, :, cols].astype(jnp.float32)
                if step:
                    total = None
                    for band in range(bands):
                        diff = values[band] - median[band]
                        total = diff * diff if total is None else total + diff * diff
                    weight = weight * lax.rsqrt(total + delta_sq)
                denom = weight if denom is None else denom + weight
                for band in range(bands):
                    term = weight * values[band]
                    numer[band] = term if numer[band] is None else numer[band] + term
            scale = 1.0 / (denom + 1.0)
            if step:
                numer = [n + m for n, m in zip(numer, median)]
            median = [n * scale for n in numer]
        for band in range(bands):
            out[band, :, cols] = median[band]


def pair_sum(terms):
    while len(terms) > 1:
        terms = [a + b for a, b in zip(terms[::2], terms[1::2])]
    return terms[0]


def sums_kernel(*refs):
    parts, out = refs[:-1], refs[-1]
    bands = parts[0].shape[0]
    for band in range(bands):
        firsts, seconds = [], []
        for part in parts:
            block = part[band]
            tiles = [block[:, c : c + LANES] for c in range(0, block.shape[1], LANES)]
            firsts.append(functools.reduce(jnp.add, tiles))
            seconds.append(functools.reduce(jnp.add, [t * t for t in tiles]))
        out[0, band : band + 1] = jnp.sum(pair_sum(firsts), axis=0, keepdims=True)
        out[1, band : band + 1] = jnp.sum(pair_sum(seconds), axis=0, keepdims=True)


def finish_kernel(count, *refs):
    sums, other, parts, out = refs[0], refs[1], refs[2:-1], refs[-1]
    bands = parts[0].shape[0]
    width = parts[0].shape[2]
    me = lax.axis_index("date")
    total = jnp.sum(sums[...] + other[...], axis=2, keepdims=True)
    mean = total[0] / count
    var = total[1] / count - mean * mean
    scale = 1.0 / jnp.sqrt(var + eps)
    for k, part in enumerate(parts):
        cols = pl.ds(pl.multiple_of((me ^ k) * width, width), width)
        for band in range(bands):
            out[band, :, cols] = (part[band] - mean[band : band + 1]) * scale[band : band + 1]


def fast_body(stack, cloud):
    _, bands, rows, cols = stack.shape
    dates = lax.axis_size("date")
    pix = lax.axis_size("pix")
    width = cols // dates
    cloudy = lambda row: (1 - row).astype(jnp.bfloat16)
    above, below = row_permutes(cloudy(cloud[:, :1]), cloudy(cloud[:, -1:]), "pix")
    shape = jax.ShapeDtypeStruct((bands + 1, rows, width), jnp.bfloat16)
    pack = call(
        pack_kernel,
        [shape] * dates,
        "pack",
        scratch_shapes=[pltpu.VMEM((rows, cols), jnp.bfloat16)],
    )
    blocks = pack(stack, cloud, above, below)
    blocks = [blocks[0]] + [swap(blocks[k], "date", k) for k in range(1, dates)]
    median = call(update_kernel, jax.ShapeDtypeStruct((bands, rows, width), jnp.float32), "update")(*blocks)
    parts = [median] + [swap(median, "date", k) for k in range(1, dates)]
    padded = -(-bands // 8) * 8
    sums = call(sums_kernel, jax.ShapeDtypeStruct((2, padded, LANES), jnp.float32), "sums")(*parts)
    bit = 1
    while bit * 2 < pix:
        sums = sums + swap(sums, "pix", bit)
        bit *= 2
    other = swap(sums, "pix", bit)
    finish = call(
        functools.partial(finish_kernel, pix * rows * cols),
        jax.ShapeDtypeStruct((bands, rows, cols), jnp.float32),
        "finish",
    )
    return finish(sums, other, *parts)


def with_halo(cells, axis, dim):
    head = lax.slice_in_dim(cells, 0, 1, axis=dim)
    tail = lax.slice_in_dim(cells, cells.shape[dim] - 1, cells.shape[dim], axis=dim)
    above, below = row_permutes(head, tail, axis)
    return jnp.concatenate([above, cells, below], axis=dim)


def plain_body(stack, cloud):
    bands, rows, cols = stack.shape[1:]
    cloudy = (1 - cloud).astype(jnp.bfloat16)
    rimmed = with_halo(cloudy, "pix", 1).astype(jnp.float32)
    padded = jnp.pad(rimmed, ((0, 0), (0, 0), (1, 1)))
    near = jnp.maximum(padded[:, 1:-1, 1:-1], padded[:, 2:, 1:-1])
    near = jnp.maximum(near, padded[:, :-2, 1:-1])
    near = jnp.maximum(near, padded[:, 1:-1, 2:])
    near = jnp.maximum(near, padded[:, 1:-1, :-2])
    valid = (1.0 - near).astype(jnp.bfloat16)
    planes = jnp.concatenate([stack, valid[:, None]], axis=1)
    planes = lax.all_to_all(planes, "date", 3, 0, tiled=True).astype(jnp.float32)
    values, valid = planes[:, :bands], planes[:, bands]
    median = jnp.zeros(values.shape[1:], jnp.float32)
    for step in range(ITERS + 1):
        weight = valid
        if step:
            diff = values - median[None]
            weight = valid / jnp.sqrt(jnp.sum(diff * diff, axis=1) + delta_sq)
        numer = jnp.sum(weight[:, None] * values, axis=0)
        denom = jnp.sum(weight, axis=0)
        median = (numer + median) / (denom + 1.0)
    median = lax.all_gather(median, "date", axis=2, tiled=True)
    count = lax.axis_size("pix") * rows * cols
    first, second = lax.psum((jnp.sum(median, axis=(1, 2)), jnp.sum(median * median, axis=(1, 2))), "pix")
    mean = first / count
    var = second / count - mean * mean
    return (median - mean[:, None, None]) / jnp.sqrt(var[:, None, None] + eps)


def body(stack, cloud):
    dates, pix = lax.axis_size("date"), lax.axis_size("pix")
    power = lambda n: n > 1 and n & (n - 1) == 0
    fits = stack.shape[0] == 1 and stack.shape[2] % 8 == 0 and stack.shape[3] % (dates * LANES) == 0
    if power(dates) and power(pix) and dates <= 16 and fits:
        return fast_body(stack, cloud)
    return plain_body(stack, cloud)


def solution(mesh):
    placed = (P("date", None, "pix", None), P("date", "pix", None))
    return jax.shard_map(
        body, mesh=mesh, in_specs=placed, out_specs=P(None, "pix", None), check_vma=False
    )
```

```python
import functools
import math

import jax
import jax.numpy as jnp
from jax import lax
from jax.experimental import pallas as pl
from jax.experimental.pallas import tpu as pltpu
from jax.sharding import PartitionSpec as P


ITERS = 2
LANES = 128

delta_sq = 0.01
eps = 1e-05

LEAST, MOST = -4.0, 12.0
CODES = 32767.0
STEPS = 1024.0
DIGIT = 32768.0
TILE = 8
CENTRE, SPREAD, MEAN, SQUARE = 0, 4, 8, 16


def row_permutes(head, tail, axis):
    count = lax.axis_size(axis)
    ends = count - 1
    above = lax.ppermute(tail, axis, [(i, i + 1) for i in range(ends)])
    below = lax.ppermute(head, axis, [(i + 1, i) for i in range(ends)])
    return above, below


def swap(x, axis, bits):
    count = lax.axis_size(axis)
    return lax.ppermute(x, axis, [(i, i ^ bits) for i in range(count)])


def ship(x, even, odd):
    dates, pix = lax.axis_size("date"), lax.axis_size("pix")
    pairs = [
        (d * pix + p, (d ^ (odd if p % 2 else even)) * pix + p)
        for d in range(dates)
        for p in range(pix)
    ]
    return lax.ppermute(x, ("date", "pix"), pairs)


def pair_rows(first, last):
    pix = lax.axis_size("pix")
    if pix == 4:
        upper = lax.axis_index("pix") < 2
        got = swap(jnp.where(upper, last, first), "pix", 2)
        return jnp.where(upper, 0.0, got), jnp.where(upper, got, 0.0)
    if pix == 2:
        return jnp.zeros_like(last), jnp.zeros_like(first)
    above = lax.ppermute(last, "pix", [(p, p + 2) for p in range(pix - 2)])
    below = lax.ppermute(first, "pix", [(p + 2, p) for p in range(pix - 2)])
    return above, below


def partners(dates):
    rest = [k for k in range(dates - 2, 1, -2) if k != dates // 2]
    return [dates // 2] + rest


VMEM = pl.BlockSpec(memory_space=pltpu.VMEM)
HBM = pl.BlockSpec(memory_space=pltpu.HBM)


def call(kernel, outs, specs=None, out_specs=None, flops=2_000_000, vmem=16, **kwargs):
    def run(*args):
        return pl.pallas_call(
            kernel,
            out_shape=outs,
            in_specs=specs or [VMEM] * len(args),
            out_specs=out_specs or jax.tree.map(lambda _: VMEM, outs),
            compiler_params=pltpu.CompilerParams(vmem_limit_bytes=vmem * 2**20),
            cost_estimate=pl.CostEstimate(flops=flops, bytes_accessed=0, transcendentals=0),
            **kwargs,
        )(*args)

    return run


def column_block(block, width):
    return pl.ds(pl.multiple_of(block * width, width), width)


def near_flags(cloudy):
    rows, cols = cloudy.shape
    line = jnp.zeros((1, cols), jnp.float32)
    edge = jnp.zeros((rows, 1), jnp.float32)
    up = jnp.concatenate([line, cloudy[:-1]], axis=0)
    down = jnp.concatenate([cloudy[1:], line], axis=0)
    left = jnp.concatenate([edge, cloudy[:, :-1]], axis=1)
    right = jnp.concatenate([cloudy[:, 1:], edge], axis=1)
    return jnp.maximum(jnp.maximum(jnp.maximum(cloudy, up), jnp.maximum(down, left)), right)


def load_kernel(stack, cloud, planes, gift, edges, flags, sems):
    bands = stack.shape[1]
    width = gift.shape[-1]
    copies = [
        pltpu.make_async_copy(cloud.at[0], flags, sems.at[0]),
        pltpu.make_async_copy(stack.at[0], planes.at[pl.ds(0, bands)], sems.at[1]),
    ]
    for copy in copies:
        copy.start()
    me = lax.axis_index("date")
    core = lax.rem(lax.axis_index("pix"), 2)
    copies[0].wait()
    cloudy = (1 - flags[...]).astype(jnp.float32)
    edges[0:1] = cloudy[:1]
    edges[1:2] = cloudy[-1:]
    planes[bands] = (1.0 - near_flags(cloudy)).astype(jnp.bfloat16)
    copies[1].wait()
    for j in range(gift.shape[0]):
        far = partners(lax.axis_size("date"))[j] + 1 - core
        cols = column_block(me ^ far, width)
        for plane in range(bands + 1):
            gift[j, plane] = planes[plane, :, cols]


def pack_kernel(planes, given, mine, other, above, below, own, last, *ships):
    bands = planes.shape[0] - 1
    width = own.shape[-1]
    rows = planes.shape[1]
    me = lax.axis_index("date")
    core = lax.rem(lax.axis_index("pix"), 2)
    row = lax.broadcasted_iota(jnp.int32, (rows, width), 0)

    def settle(flags, cols, lower, neighbour):
        over = jnp.where(lower, neighbour[1:2, cols], above[:, cols])
        under = jnp.where(lower, below[:, cols], neighbour[0:1, cols])
        cloudy = jnp.maximum(
            jnp.where(row == 0, over, 0.0), jnp.where(row == rows - 1, under, 0.0)
        )
        return (flags.astype(jnp.float32) * (1.0 - cloudy)).astype(jnp.bfloat16)

    def own_block(out, block):
        cols = column_block(block, width)
        for band in range(bands):
            out[band] = planes[band, :, cols]
        out[bands] = settle(planes[bands, :, cols], cols, core == 1, other)

    own_block(own, me)
    own_block(last, me ^ 1)
    for j, out in enumerate(ships):
        block = me ^ (partners(lax.axis_size("date"))[j] + core)
        own_block(out.at[0], block)
        cols = column_block(block, width)
        for band in range(bands):
            out[1, band] = given[j, band]
        out[1, bands] = settle(given[j, bands], cols, core == 0, mine)


def span(rows, width):
    limit = 1.02 * math.sqrt(rows * width)
    return limit / math.sqrt(1.0 + limit)


def nearest(x):
    return jnp.clip(jnp.floor(x + 0.5), -CODES, CODES)


def digits(x, unit, count):
    found = []
    x = x * (1.0 / unit)
    for _ in range(count):
        found.append(nearest(x))
        x = (x - found[-1]) * DIGIT
    return found


def weights(lane, start, unit, count):
    out = jnp.zeros(lane.shape, jnp.float32)
    for i in range(count):
        out = jnp.where(lane == start + i, unit / DIGIT**i, out)
    return out


MIDDLE = (MOST + LEAST) / 2
UNIT = (MOST - LEAST) / 2 / CODES
SQUARE_UNIT = max(LEAST * LEAST, MOST * MOST) / CODES


def spread_of(code):
    return jnp.exp(code * (math.log(2.0) / STEPS))


def as_float(codes):
    return codes.astype(jnp.int32).astype(jnp.float32)


def as_codes(x):
    return x.astype(jnp.int32).astype(jnp.int16)


def over_lanes(x):
    return jnp.broadcast_to(jnp.sum(x, axis=1, keepdims=True), x.shape)


def add_tiles(block):
    tiles = [block[:, c : c + LANES] for c in range(0, block.shape[1], LANES)]
    return jnp.sum(functools.reduce(jnp.add, tiles), axis=0, keepdims=True)


def update_kernel(rounds, *refs):
    out, moments = refs[-2:]
    parts = list(refs[:-2])
    parts = parts[:2] + [r.at[0] for r in parts[2 : 2 + rounds]] + parts[2 + rounds :]
    bands, rows, width = out.shape
    for first in range(0, width, LANES):
        cols = pl.ds(first, LANES)
        median = None
        for step in range(ITERS + 1):
            numer, denom = [None] * bands, None
            for part in parts:
                values = [part[band, :, cols].astype(jnp.float32) for band in range(bands)]
                weight = part[bands, :, cols].astype(jnp.float32)
                if step:
                    total = None
                    for band in range(bands):
                        diff = values[band] - median[band]
                        total = diff * diff if total is None else total + diff * diff
                    weight = weight * lax.rsqrt(total + delta_sq)
                denom = weight if denom is None else denom + weight
                for band in range(bands):
                    term = weight * values[band]
                    numer[band] = term if numer[band] is None else numer[band] + term
            scale = 1.0 / (denom + 1.0)
            if step:
                numer = [n + m for n, m in zip(numer, median)]
            median = [n * scale for n in numer]
        for band in range(bands):
            out[band, :, cols] = median[band]
    moments[...] = jnp.zeros_like(moments)
    for band in range(bands):
        x = out[band]
        moments[0, band : band + 1] = add_tiles(x)
        moments[1, band : band + 1] = add_tiles(x * x)
    for i in range(2):
        moments[i] = over_lanes(moments[i]) * (1.0 / (rows * width))


def encode_kernel(block, moments, out, squares, table):
    bands, rows, width = block.shape
    top = span(rows, width)
    lane = lax.broadcasted_iota(jnp.int32, squares.shape, 1)
    centre = digits(moments[0] - MIDDLE, UNIT, 2)
    table[0] = MIDDLE + UNIT * centre[0] + (UNIT / DIGIT) * centre[1]
    squares[...] = jnp.zeros_like(squares)
    for band in range(bands):
        off = block[band] - jnp.broadcast_to(table[0, band : band + 1, :1], (rows, width))
        squares[band : band + 1] = add_tiles(off * off)
    square = over_lanes(squares[...]) * (1.0 / (rows * width))
    size = jnp.ceil(jnp.log(jnp.maximum(square, 1e-18)) * (STEPS / (2 * math.log(2.0))))
    table[1] = 1.0 / spread_of(size)
    sides = jnp.where(lane == CENTRE, centre[0], jnp.where(lane == CENTRE + 1, centre[1], 0.0))
    sides = as_codes(jnp.where(lane == SPREAD, size, sides))
    for group in range(squares.shape[0] // TILE):
        out[bands, :, group * LANES : (group + 1) * LANES] = sides[group * TILE : (group + 1) * TILE]
    for c in range(squares.shape[0] // TILE * LANES, width, LANES):
        out[bands, :, c : c + LANES] = jnp.zeros((rows, LANES), jnp.int16)
    for band in range(bands):
        middle = jnp.broadcast_to(table[0, band : band + 1], (rows, LANES))
        shrink = jnp.broadcast_to(table[1, band : band + 1], (rows, LANES))
        for c in range(0, width, LANES):
            u = (block[band, :, c : c + LANES] - middle) * shrink
            code = nearest(u * lax.rsqrt(1.0 + jnp.abs(u)) * (CODES / top))
            out[band, :, c : c + LANES] = as_codes(code)


def join_kernel(pairs, mine, other, moments, more, out):
    bands = mine.shape[0] - 1
    both = (moments[...] + more[...]) * (1.0 / pairs)
    lane = lax.broadcasted_iota(jnp.int32, both.shape[1:], 1)
    sides = jnp.zeros(both.shape[1:], jnp.float32)
    for i, d in enumerate(digits(both[0] - MIDDLE, UNIT, 3)):
        sides = jnp.where(lane == MEAN + i, d, sides)
    for i, d in enumerate(digits(both[1], SQUARE_UNIT, 3)):
        sides = jnp.where(lane == SQUARE + i, d, sides)
    for half, block in enumerate((mine, other)):
        out[half] = block[...]
        for group in range(both.shape[1] // TILE):
            cols = slice(group * LANES, (group + 1) * LANES)
            flags = as_float(block[bands, :, cols]) + sides[group * TILE : (group + 1) * TILE]
            out[half, bands, :, cols] = as_codes(flags)


def by_distance(dates, core, parts):
    rounds = partners(dates)
    own, last, ships, passed = parts[0], parts[1], parts[2 : 2 + len(rounds)], parts[2 + len(rounds) :]
    found = [(0, own), (1, last)]
    for k, direct, other in zip(rounds, ships, passed):
        found += [(k + core, direct.at[0]), (k + 1 - core, other)]
    return found


def finish_kernel(*refs):
    parts, out, result, table, sems = refs[:-4], refs[-4], refs[-3], refs[-2], refs[-1]
    bands, rows, width = parts[0].shape[0] - 1, parts[0].shape[1], parts[0].shape[2]
    top = span(rows, width)
    groups = table.shape[1] // TILE
    me = lax.axis_index("date")
    core = lax.rem(lax.axis_index("pix"), 2)
    dates = lax.axis_size("date")
    lane = lax.broadcasted_iota(jnp.int32, (rows, LANES), 1)
    blocks = by_distance(dates, core, parts)
    for group in range(groups):
        cols = slice(group * LANES, (group + 1) * LANES)
        sides = [as_float(part[bands, :, cols]) for _, part in blocks]
        total = functools.reduce(jnp.add, sides) * (1.0 / dates)
        mean = over_lanes(total * weights(lane, MEAN, UNIT, 3)) + MIDDLE
        var = over_lanes(total * weights(lane, SQUARE, SQUARE_UNIT, 3)) - mean * mean
        scale = 1.0 / jnp.sqrt(var + eps)
        for i, side in enumerate(sides):
            centre = over_lanes(side * weights(lane, CENTRE, UNIT, 2)) + MIDDLE
            spread = spread_of(over_lanes(side * weights(lane, SPREAD, 1.0, 1)))
            place = slice(group * TILE, (group + 1) * TILE)
            table[2 * i, place] = (0.5 * spread) * scale
            table[2 * i + 1, place] = (centre - mean) * scale
    copies = []
    for i, (far, part) in enumerate(blocks):
        first = pl.multiple_of((me ^ far) * width, width)
        for band in range(bands):
            gain = jnp.broadcast_to(table[2 * i, band : band + 1], (rows, LANES))
            base = jnp.broadcast_to(table[2 * i + 1, band : band + 1], (rows, LANES))
            for c in range(0, width, LANES):
                y = as_float(part[band, :, c : c + LANES]) * (top / CODES)
                z = y * y + 4.0
                u = y * (jnp.abs(y) + z * lax.rsqrt(z))
                result[i, band, :, c : c + LANES] = u * gain + base
        copies.append(
            pltpu.make_async_copy(result.at[i], out.at[:, :, pl.ds(first, width)], sems.at[i])
        )
        copies[-1].start()
    for copy in copies:
        copy.wait()


def exchange(ships, last):
    rounds = partners(lax.axis_size("date"))
    found = []
    for x, k in zip(ships, rounds):
        found.append(ship(x, k, k + 1))
    last = swap(last, "date", 1)
    passed = [swap(x[1], "pix", 1) for x in found]
    return found, last, passed


def fast_body(stack, cloud):
    _, bands, rows, cols = stack.shape
    dates = lax.axis_size("date")
    pix = lax.axis_size("pix")
    width = cols // dates
    rounds = partners(dates)
    half = jax.ShapeDtypeStruct((bands + 1, rows, width), jnp.bfloat16)
    upper = lax.axis_index("pix") % 2 == 0
    load = call(
        load_kernel,
        [
            jax.ShapeDtypeStruct((bands + 1, rows, cols), jnp.bfloat16),
            jax.ShapeDtypeStruct((len(rounds),) + half.shape, jnp.bfloat16),
            jax.ShapeDtypeStruct((2, cols), jnp.float32),
        ],
        [HBM, HBM],
        vmem=40,
        scratch_shapes=[pltpu.VMEM((rows, cols), jnp.int32), pltpu.SemaphoreType.DMA((2,))],
    )
    planes, gift, mine = load(stack, cloud)
    other = swap(mine, "pix", 1)
    given = swap(gift, "pix", 1)
    above, below = pair_rows(
        jnp.where(upper, mine[:1], other[:1]), jnp.where(upper, other[1:], mine[1:])
    )
    both = jax.ShapeDtypeStruct((2,) + half.shape, jnp.bfloat16)
    pack = call(pack_kernel, [half, half] + [both] * len(rounds))
    own, last, *ships = pack(planes, given, mine, other, above, below)
    ships, last, passed = exchange(ships, last)
    groups = -(-bands // TILE) * TILE
    table = jax.ShapeDtypeStruct((2, groups, LANES), jnp.float32)
    update = call(
        functools.partial(update_kernel, len(rounds)), [jax.ShapeDtypeStruct((bands, rows, width), jnp.float32), table]
    )
    median, moments = update(own, last, *ships, *passed)
    total = moments
    bit = 1
    while bit * 2 < pix:
        total = total + swap(total, "pix", bit)
        bit *= 2
    more = swap(total, "pix", bit)
    encode = call(
        encode_kernel,
        jax.ShapeDtypeStruct(half.shape, jnp.int16),
        scratch_shapes=[pltpu.VMEM((groups, LANES), jnp.float32), pltpu.VMEM(table.shape, jnp.float32)],
    )
    coded = encode(median, moments)
    join = call(functools.partial(join_kernel, pix), jax.ShapeDtypeStruct(both.shape, jnp.int16))
    pair = join(coded, swap(coded, "pix", 1), total, more)
    own = pair[0]
    ships, last, passed = exchange([pair] * len(rounds), own)
    finish = call(
        finish_kernel,
        jax.ShapeDtypeStruct((bands, rows, cols), jnp.float32),
        out_specs=HBM,
        scratch_shapes=[
            pltpu.VMEM((dates, bands, rows, width), jnp.float32),
            pltpu.VMEM((2 * dates, groups, LANES), jnp.float32),
            pltpu.SemaphoreType.DMA((dates,)),
        ],
    )
    return finish(own, last, *ships, *passed)


def with_halo(cells, axis, dim):
    head = lax.slice_in_dim(cells, 0, 1, axis=dim)
    tail = lax.slice_in_dim(cells, cells.shape[dim] - 1, cells.shape[dim], axis=dim)
    above, below = row_permutes(head, tail, axis)
    return jnp.concatenate([above, cells, below], axis=dim)


def plain_body(stack, cloud):
    bands, rows, cols = stack.shape[1:]
    cloudy = (1 - cloud).astype(jnp.bfloat16)
    rimmed = with_halo(cloudy, "pix", 1).astype(jnp.float32)
    padded = jnp.pad(rimmed, ((0, 0), (0, 0), (1, 1)))
    near = jnp.maximum(padded[:, 1:-1, 1:-1], padded[:, 2:, 1:-1])
    near = jnp.maximum(near, padded[:, :-2, 1:-1])
    near = jnp.maximum(near, padded[:, 1:-1, 2:])
    near = jnp.maximum(near, padded[:, 1:-1, :-2])
    valid = (1.0 - near).astype(jnp.bfloat16)
    planes = jnp.concatenate([stack, valid[:, None]], axis=1)
    planes = lax.all_to_all(planes, "date", 3, 0, tiled=True).astype(jnp.float32)
    values, valid = planes[:, :bands], planes[:, bands]
    median = jnp.zeros(values.shape[1:], jnp.float32)
    for step in range(ITERS + 1):
        weight = valid
        if step:
            diff = values - median[None]
            weight = valid / jnp.sqrt(jnp.sum(diff * diff, axis=1) + delta_sq)
        numer = jnp.sum(weight[:, None] * values, axis=0)
        denom = jnp.sum(weight, axis=0)
        median = (numer + median) / (denom + 1.0)
    median = lax.all_gather(median, "date", axis=2, tiled=True)
    count = lax.axis_size("pix") * rows * cols
    first, second = lax.psum((jnp.sum(median, axis=(1, 2)), jnp.sum(median * median, axis=(1, 2))), "pix")
    mean = first / count
    var = second / count - mean * mean
    return (median - mean[:, None, None]) / jnp.sqrt(var[:, None, None] + eps)


def is_fast(dates, pix, local, bands, rows, cols):
    power = all(n > 1 and n & (n - 1) == 0 for n in (dates, pix))
    width = cols // dates
    fits = local == 1 and rows == TILE and width % LANES == 0 and bands <= TILE * (width // LANES)
    return power and fits and cols % dates == 0 and 4 <= dates <= 16


def body(stack, cloud):
    local, bands, rows, cols = stack.shape
    if is_fast(lax.axis_size("date"), lax.axis_size("pix"), local, bands, rows, cols):
        return fast_body(stack, cloud)
    return plain_body(stack, cloud)


def solution(mesh):
    placed = (P("date", None, "pix", None), P("date", "pix", None))
    return jax.shard_map(
        body, mesh=mesh, in_specs=placed, out_specs=P(None, "pix", None), check_vma=False
    )
```
